32 devices in a mesh: groups: 2 (over x), row: 8 (over z, y), head: 2 (over core).
Axes of the slice: x: 2, y: 2, z: 4, core: 2. Of those that a mesh axis runs over, the one named last changes fastest.
Arguments:
- hidden: bfloat16 [48, 4096], P('groups'), parts along dimension 0, may hold values from -6 to 6
- norm_gain: float32 [4096], replicated, may hold values from 0.1 to 1.9
- w_query: bfloat16 [8, 256, 4096], P('head', 'row'), may hold values from -0.09375 to 0.09375
- w_key: bfloat16 [8, 256, 4096], P('head', 'row'), may hold values from -0.09375 to 0.09375
- w_value: bfloat16 [8, 512, 4096], P('head', 'row'), may hold values from -0.09375 to 0.09375
- w_outgate: bfloat16 [8, 512, 4096], P('head', 'row'), may hold values from -0.09375 to 0.09375
- w_out: bfloat16 [8, 512, 4096], P('head', 'row'), may hold values from -0.125 to 0.125
- w_gates: bfloat16 [2, 8, 4096], P(None, 'head'), may hold values from -0.09375 to 0.09375
- gate_bias: float32 [2, 8], P(None, 'head'), may hold values from -2 to 4
- headnorm_gain: float32 [8, 512], P('head', 'row'), may hold values from 0.1 to 1.9
- final_gain: float32 [4096], replicated, may hold values from 0.1 to 1.9
- w_vocab: bfloat16 [25152, 4096], P(('row', 'head')), may hold values from -39.0625 to 39.0625
- memory: float32 [48, 8, 256, 512], P('groups', 'head', 'row'), parts along dimension 0, may hold values from -6 to 6
- normalizer: float32 [48, 8, 256], P('groups', 'head', 'row'), parts along dimension 0, may hold values from -6 to 6
- stabilizer: float32 [48, 8], P('groups', 'head'), parts along dimension 0, may hold values from -2 to 2
- targets: int32 [48], P('groups'), parts along dimension 0, may hold values from 0 to 25151
Outputs:
- memory_out: float32 [48, 8, 256, 512], P('groups', 'head', 'row'), parts along dimension 0
- normalizer_out: float32 [48, 8, 256], P('groups', 'head', 'row'), parts along dimension 0
- stabilizer_out: float32 [48, 8], P('groups', 'head'), parts along dimension 0
- hidden_out: bfloat16 [48, 4096], P('groups', ('row', 'head')), parts along dimension 0
- log_prob: float32 [48], P('groups'), parts along dimension 0
The draws below stay inside these ranges and needn't reach their ends.
There are 2 independent parts, one for each index of `groups`. The reference program is written for one: setup_inputs(seed, part) draws one part's arguments, and reference() takes and returns one part's arrays. A program takes and returns all parts, laid end to end along the dimension named above; an argument that names none is the same for every part. Nothing has to cross between parts.
All inputs are finite; a program needn't handle non-finite values.
Results may differ from the reference program's by a relative error of at most 0.0035.
The reference program's roundings to bfloat16 on the way (of `normed_in`, `value_part`, `gated_out` and `final_feat`) count: a program that leaves them out, or rounds other values in their place, can miss the bound.
Values may be sent and summed in bfloat16 or wider, within the bound.
A program may use at most 64 MiB of HBM per device.

```python
import math
import jax
import jax.numpy as jnp
import numpy as np
from jax import lax

D = 4096
HEADS = 8
QK_DIM = 256
HEAD_DIM = 512
VOCAB = 25152
SEQ = 24


def draw_w_vocab(key, part):
    drawn_rows = jnp.clip(jax.random.normal(jax.random.fold_in(key, 11), (VOCAB, D), jnp.float32), -6.0, 6.0) / math.sqrt(D)
    return drawn_rows.astype(jnp.bfloat16)


def set_ends(array, stream_key, least, high):
    spot = [jax.random.randint(jax.random.fold_in(stream_key, axis), (), 0, length) for axis, length in enumerate(array.shape)]
    widest = array.shape.index(max(array.shape))
    next_to = spot[:widest] + [(spot[widest] + 1) % array.shape[widest]] + spot[widest + 1:]
    return array.at[tuple(spot)].set(least).at[tuple(next_to)].set(high)


def with_spikes(array, own_key, source, target, shards_of, factor):
    def block_of(position):
        return (jnp.arange(array.shape[position]) // (array.shape[position] // shards_of)).reshape((-1,) + (1,) * (array.ndim - 1 - position))

    near = jax.random.permutation(own_key, shards_of)[block_of(target)]
    second = (block_of(target) + shards_of // 2) % shards_of
    return jnp.where((block_of(source) == near) | (block_of(source) == second), factor * array, array)


def steps_of(rng, shape, cuts, least, high):
    factor_of, own = 1.0, jax.random.fold_in(rng, 6)
    for position, shards_of in cuts:
        draws = jnp.exp(jax.random.uniform(jax.random.fold_in(own, position), (shards_of,), jnp.float32, least / len(cuts), high / len(cuts)))
        factor_of = factor_of * jnp.repeat(draws, shape[position] // shards_of).reshape([-1 if axis == position else 1 for axis in range(len(shape))])
    return factor_of


def cumulative_ranks(number_of, lean):
    weights = [(1 << 20) // math.isqrt(rank ** lean) + 1 for rank in range(1, number_of + 1)]
    spread = 1 + sum(weights) // (1 << 30)
    return np.cumsum(np.array([max(1, weight // spread) for weight in weights]))


def ranked(own_key, shape, amount, skew):
    grid = cumulative_ranks(amount, skew)
    ticket = jax.random.randint(jax.random.fold_in(own_key, 1), shape, 0, int(grid[amount - 1]))
    rank = jnp.searchsorted(jnp.asarray(grid, jnp.int32), ticket, side="right")
    return jax.random.permutation(jax.random.fold_in(own_key, 2), amount)[rank].astype(jnp.int32)


def normal_values(own_key, extent, spread, most, shards=(), kind=jnp.bfloat16):
    array = jax.random.normal(own_key, extent, jnp.float32) * spread
    if len(shards) > 0:
        array = steps_of(own_key, extent, shards, -0.22, 0.18) * array
    return jnp.clip(array, min=-most, max=most).astype(kind)


def noise_with(rng, extent, spread, bound, pieces, heavy, held_as=jnp.bfloat16):
    entries = spread * jax.random.normal(rng, extent, jnp.float32)
    if pieces:
        entries = entries * steps_of(rng, extent, pieces, -0.22, 0.18)
    return jnp.clip(with_spikes(entries, jax.random.fold_in(rng, 3), *heavy), -bound, bound).astype(held_as)


def setup_inputs(seed: int = 0, part: int = 0) -> dict:
    key_of = jax.random.split(jax.random.key(seed), 17)
    part_keys = jax.random.split(jax.random.fold_in(key_of[16], part), 17)
    return {
        "hidden": normal_values(part_keys[0], (SEQ, D), 1.0, 6.0),
        "norm_gain": jnp.clip(1.0 + 0.18 * jax.random.normal(key_of[1], (D,), jnp.float32), 0.1, 1.9),
        "w_query": normal_values(key_of[2], (HEADS, QK_DIM, D), D ** -0.5, 0.09375, ((0, 2), (1, 8))),
        "w_key": normal_values(key_of[3], (HEADS, QK_DIM, D), D ** -0.5, 0.09375, ((0, 2), (1, 8))),
        "w_value": normal_values(key_of[4], (HEADS, HEAD_DIM, D), D ** -0.5, 0.09375, ((0, 2), (1, 8))),
        "w_outgate": normal_values(key_of[5], (HEADS, HEAD_DIM, D), D ** -0.5, 0.09375, ((0, 2), (1, 8))),
        "w_out": noise_with(key_of[6], (HEADS, HEAD_DIM, D), (HEADS * HEAD_DIM) ** -0.5, 0.125, ((0, 2), (1, 8)), (1, 2, 8, 2.0)),
        "w_gates": normal_values(key_of[7], (2, HEADS, D), D ** -0.5, 0.09375, ((1, 2),)),
        "gate_bias": jnp.clip(-2.0 + 6.0 * jax.random.uniform(key_of[8], (2, HEADS), jnp.float32) ** steps_of(key_of[8], (2, HEADS), ((1, 2),), -0.2, 0.2), -2.0, 4.0),
        "headnorm_gain": jnp.clip(1.0 + 0.18 * jax.random.normal(key_of[9], (HEADS, HEAD_DIM), jnp.float32), 0.1, 1.9),
        "final_gain": jnp.clip(1.0 + 0.18 * jax.random.normal(key_of[10], (D,), jnp.float32), 0.1, 1.9),
        "w_vocab": draw_w_vocab(jax.random.fold_in(key_of[16], 71), part),
        "memory": normal_values(part_keys[12], (SEQ, HEADS, QK_DIM, HEAD_DIM), 1.0, 6.0, ((1, 2), (2, 8)), jnp.float32),
        "normalizer": normal_values(part_keys[13], (SEQ, HEADS, QK_DIM), 1.0, 6.0, ((1, 2), (2, 8)), jnp.float32),
        "stabilizer": jnp.clip(jax.random.uniform(part_keys[14], (SEQ, HEADS), jnp.float32, -2.0, 2.0) * steps_of(part_keys[14], (SEQ, HEADS), ((1, 2),), -0.4, 0.0), -2.0, 2.0),
        "targets": set_ends(ranked(part_keys[15], (SEQ,), VOCAB, 2), jax.random.fold_in(part_keys[15], 3), 0, VOCAB - 1).astype(jnp.int32),
    }


epsilon = 1e-06

def rms_round(stream, gain):
    scale = lax.rsqrt(lax.optimization_barrier(jnp.mean(stream * stream, axis=-1, keepdims=True)) + epsilon)
    return (stream * scale * gain).astype(jnp.bfloat16)

def reference(hidden, norm_gain, w_query, w_key, w_value, w_outgate, w_out, w_gates, gate_bias, headnorm_gain, final_gain, w_vocab, memory, normalizer, stabilizer, targets):
    stream = hidden.astype(jnp.float32)
    normed_in = rms_round(stream, norm_gain)
    inputs = lax.optimization_barrier(normed_in).astype(jnp.float32)

    def project(weights):
        return jnp.einsum('sd,hjd->shj', inputs, weights.astype(jnp.float32))
    queries = project(w_query) / math.sqrt(QK_DIM)
    key_part = project(w_key)
    value_part = lax.optimization_barrier(project(w_value).astype(jnp.bfloat16)).astype(jnp.float32)
    outgate_pre = project(w_outgate)
    gate_pre = jnp.einsum('sd,ghd->gsh', inputs, w_gates.astype(jnp.float32)) + gate_bias[:, None, :]
    log_forget = jax.nn.log_sigmoid(gate_pre[1])
    stabilizer_out = jnp.maximum(log_forget + stabilizer, gate_pre[0])
    decay_rate = jnp.exp(log_forget + stabilizer - stabilizer_out)
    inflow = jnp.exp(gate_pre[0] - stabilizer_out)
    scaled_key = inflow[:, :, None] * key_part
    memory_out = decay_rate[:, :, None, None] * memory + scaled_key[:, :, :, None] * value_part[:, :, None, :]
    normalizer_out = decay_rate[:, :, None] * normalizer + scaled_key
    readout = jnp.einsum('shj,shje->she', queries, memory_out, precision=lax.Precision.HIGHEST)
    average = lax.optimization_barrier(jnp.mean(readout, axis=-1, keepdims=True))
    centered = readout - average
    variance = lax.optimization_barrier(jnp.mean(centered * centered, axis=-1, keepdims=True))
    normed = centered * lax.rsqrt(variance + epsilon) * headnorm_gain
    gated_out = (jax.nn.sigmoid(outgate_pre) * normed).astype(jnp.bfloat16)
    projection = jnp.einsum('shj,hjd->sd', lax.optimization_barrier(gated_out).astype(jnp.float32), w_out.astype(jnp.float32))
    hidden_out = (stream + projection).astype(jnp.bfloat16)
    final_feat = rms_round(hidden_out.astype(jnp.float32), final_gain)
    logits = jnp.dot(final_feat, w_vocab.T, preferred_element_type=jnp.float32)
    highest = lax.optimization_barrier(jnp.max(logits, axis=-1))
    log_total = highest + jnp.log(lax.optimization_barrier(jnp.sum(jnp.exp(logits - highest[:, None]), axis=-1)))
    picked = jnp.take_along_axis(logits, targets.astype(jnp.int32)[:, None], axis=1)[:, 0]
    return (memory_out, normalizer_out, stabilizer_out, hidden_out, picked - log_total)
```

```python
import functools
import math

import jax
import jax.numpy as jnp
from jax import lax
from jax.experimental import pallas as pl
from jax.experimental.pallas import tpu as pltpu
from jax.sharding import PartitionSpec as P

epsilon = 1e-06
LANES = 128
MESH = pl.DeviceIdType.MESH


def dot_nt(left, right):
    return lax.dot_general(left, right, (((1,), (1,)), ((), ())), preferred_element_type=jnp.float32)


def lane_of(shape):
    return lax.broadcasted_iota(jnp.int32, shape, len(shape) - 1)


def spread(columns, width, count):
    head_of = lane_of((columns.shape[0], width * count)) // width
    total = jnp.zeros((columns.shape[0], width * count), jnp.float32)
    for h in range(count):
        total = jnp.where(head_of == h, columns[:, h : h + 1], total)
    return total


def segment_sums(values, width, count):
    head_of = lane_of(values.shape) // width
    return [jnp.sum(jnp.where(head_of == h, values, 0.0), axis=-1, keepdims=True) for h in range(count)]


def as_rows(columns):
    seqs = columns[0].shape[0]
    lane = lane_of((seqs, LANES))
    wide = jnp.zeros((seqs, LANES), jnp.float32)
    for i, column in enumerate(columns):
        wide = jnp.where(lane == i, column, wide)
    return jnp.transpose(wide)[0:8, :]


def kernel(
    rows, cores, heads,
    hidden, norm_gain, w_query, w_key, w_value, w_outgate, w_out, w_gates, gate_bias, headnorm, final_gain,
    w_vocab, memory, stabilizer, targets,
    values_out, key_out, decay_out, stabilizer_out, hidden_out, log_prob,
    wq, wk, wv, wg, wo, wvoc, mem,
    q_cols, part, readout, read_send, read_in, qk_in, stat_in, proj, pair_in, proj_send, proj_in, share, own_share,
    joined, last_in, small_send,
    load_sem, v_send, v_recv, qk_send, qk_recv, rd_send, rd_recv, st_send, st_recv,
    pa_send, pa_recv, pr_send, pr_recv, ag_send, ag_recv, fw_send, fw_recv, ls_send, ls_recv,
):
    seqs, model = hidden.shape
    r = lax.axis_index("row")
    c = lax.axis_index("head")
    other = 1 - c
    spot = r * cores + c
    keys = w_query.shape[1]
    vals = w_value.shape[1]
    head_dim = memory.shape[3]
    width = share.shape[3]

    loads = [
        pltpu.make_async_copy(source, target, load_sem.at[i])
        for i, (source, target) in enumerate(
            ((w_key, wk), (w_query, wq), (memory, mem), (w_value, wv), (w_outgate, wg), (w_out, wo), (w_vocab, wvoc))
        )
    ]
    for load in loads[:5]:
        load.start()

    barrier = pltpu.get_barrier_semaphore()
    for k in range(1, rows * cores):
        to = lax.rem(spot + k, rows * cores)
        pl.semaphore_signal(
            barrier, inc=1, device_id={"row": to // cores, "head": lax.rem(to, cores)}, device_id_type=MESH
        )

    def to_rows(source_of, target, send, recv):
        out, back = [], []
        for k in range(1, rows):
            to = lax.rem(r + k, rows)
            come = lax.rem(r + rows - k, rows)
            where = {"row": to, "head": c}
            copy = pltpu.make_async_remote_copy(
                src_ref=source_of(to), dst_ref=target.at[r], send_sem=send.at[k], recv_sem=recv.at[k],
                device_id=where, device_id_type=MESH,
            )
            copy.start()
            out.append(copy)
            back.append(
                pltpu.make_async_remote_copy(
                    src_ref=source_of(to), dst_ref=target.at[come], send_sem=send.at[k], recv_sem=recv.at[k],
                    device_id=where, device_id_type=MESH,
                )
            )
        return out, back

    stream = hidden[...].astype(jnp.float32)
    scale = lax.rsqrt(jnp.mean(stream * stream, axis=-1, keepdims=True) + epsilon)
    x = (stream * scale * norm_gain[...]).astype(jnp.bfloat16)
    gate_in = dot_nt(x, w_gates[0]) + gate_bias[0:1, :]
    gate_forget = dot_nt(x, w_gates[1]) + gate_bias[1:2, :]
    log_forget = jnp.minimum(gate_forget, 0.0) - jnp.log1p(jnp.exp(-jnp.abs(gate_forget)))
    top = jnp.maximum(log_forget + stabilizer[...], gate_in)
    decay = jnp.exp(log_forget + stabilizer[...] - top)
    inflow = jnp.exp(gate_in - top)
    stabilizer_out[...] = top
    decay_out[...] = decay

    loads[0].wait()
    key = dot_nt(x, wk[...].reshape(heads * keys, model)) * spread(inflow, keys, heads)
    key_out[...] = key
    loads[1].wait()
    query = dot_nt(x, wq[...].reshape(heads * keys, model)) / math.sqrt(rows * keys)
    query_t = jnp.transpose(query)
    for s in range(seqs):
        q_cols[s] = jnp.broadcast_to(query_t[:, s : s + 1], (heads * keys, LANES))
    small_send[0] = as_rows(segment_sums(query * key, keys, heads))
    qk_in[r] = small_send[0]
    pl.semaphore_wait(barrier, rows * cores - 1)
    qk_out, qk_back = to_rows(lambda to: small_send.at[0], qk_in, qk_send, qk_recv)

    loads[2].wait()

    sublane = lax.broadcasted_iota(jnp.int32, (8, LANES), 0)

    def read(group, carry):
        for h in range(heads):
            for t in range(head_dim // LANES):
                stack = jnp.zeros((8, LANES), jnp.float32)
                for i in range(8):
                    s = group * 8 + i
                    q = q_cols[s, h * keys : (h + 1) * keys, :]
                    block = mem[s, h, :, t * LANES : (t + 1) * LANES]
                    stack = jnp.where(sublane == i, jnp.sum(q * block, axis=0, keepdims=True), stack)
                first = pl.multiple_of(group * 8, 8)
                readout[h, pl.ds(first, 8), t * LANES : (t + 1) * LANES] = stack
        return carry

    lax.fori_loop(0, seqs // 8, read, 0)
    low = lane_of((seqs, LANES)) < vals
    for pair in range(heads // 2):
        for t in range(head_dim // LANES):
            tile = slice(t * LANES, (t + 1) * LANES)
            a = readout[2 * pair, :, tile] * decay[:, 2 * pair : 2 * pair + 1]
            b = readout[2 * pair + 1, :, tile] * decay[:, 2 * pair + 1 : 2 * pair + 2]
            here = slice(pair * LANES, (pair + 1) * LANES)
            read_send[2 * t, :, here] = jnp.where(low, a, pltpu.roll(b, vals, 1))
            read_send[2 * t + 1, :, here] = jnp.where(low, pltpu.roll(a, vals, 1), b)
    read_in[r] = read_send[r]
    rd_out, rd_back = to_rows(lambda to: read_send.at[to], read_in, rd_send, rd_recv)

    loads[3].wait()
    value = dot_nt(x, wv[...].reshape(heads * vals, model)).astype(jnp.bfloat16)
    part[...] = value
    values_out[r] = value
    v_out, v_back = to_rows(lambda to: part, values_out, v_send, v_recv)
    loads[5].start()
    loads[6].start()
    loads[4].wait()
    gate = jax.nn.sigmoid(dot_nt(x, wg[...].reshape(heads * vals, model)))

    for copy in qk_back:
        copy.wait_recv()
    qk_rows = qk_in[0]
    for i in range(1, rows):
        qk_rows = qk_rows + qk_in[i]
    qk = jnp.transpose(jnp.concatenate([qk_rows] + [jnp.zeros_like(qk_rows)] * (LANES // 8 - 1), axis=0))
    value_term = spread(qk, vals, heads) * value.astype(jnp.float32)

    for copy in rd_back:
        copy.wait_recv()
    read_full = value_term
    for i in range(rows):
        read_full = read_full + read_in[i]
    means = [total / vals for total in segment_sums(read_full, vals, heads)]
    local_mean = spread(jnp.concatenate(means, axis=1), vals, heads)
    offs = read_full - local_mean
    small_send[1] = as_rows(means + segment_sums(offs * offs, vals, heads))
    stat_in[r] = small_send[1]
    st_out, st_back = to_rows(lambda to: small_send.at[1], stat_in, st_send, st_recv)
    for copy in st_back:
        copy.wait_recv()
    average = stat_in[0, 0:heads]
    spreads = stat_in[0, heads : 2 * heads]
    for i in range(1, rows):
        average = average + stat_in[i, 0:heads]
        spreads = spreads + stat_in[i, heads : 2 * heads]
    average = average / rows
    for i in range(rows):
        off = stat_in[i, 0:heads] - average
        spreads = spreads + vals * off * off
    inverse = lax.rsqrt(spreads / head_dim + epsilon)
    both = jnp.concatenate([average, inverse], axis=0)
    both = jnp.transpose(jnp.concatenate([both] + [jnp.zeros_like(both)] * (LANES // 8 - 1), axis=0))
    normed = (read_full - spread(both, vals, heads)) * spread(both[:, heads:], vals, heads) * headnorm[...]
    gated = (gate * normed).astype(jnp.bfloat16)

    loads[5].wait()
    for i in range(rows):
        for j in range(cores):
            at = (i * cores + j) * width
            proj[j, i] = jnp.dot(
                gated, wo[:, :, at : at + width].reshape(heads * vals, width), preferred_element_type=jnp.float32
            )
    pair_copy = pltpu.make_async_remote_copy(
        src_ref=proj.at[other], dst_ref=pair_in, send_sem=pa_send, recv_sem=pa_recv,
        device_id={"row": r, "head": other}, device_id_type=MESH,
    )
    pair_copy.start()
    pair_copy.wait_recv()
    for i in range(rows):
        proj_send[i] = proj[c, i] + pair_in[i]
    proj_in[r] = proj_send[r]
    pr_out, pr_back = to_rows(lambda to: proj_send.at[to], proj_in, pr_send, pr_recv)
    for copy in pr_back:
        copy.wait_recv()
    new = proj_in[0]
    for i in range(1, rows):
        new = new + proj_in[i]
    mine = hidden[:, pl.ds(pl.multiple_of(spot * width, LANES), width)].astype(jnp.float32)
    new = (mine + new).astype(jnp.bfloat16)
    hidden_out[...] = new
    own_share[...] = new
    share[c, r] = new
    ag_out, ag_back = to_rows(lambda to: own_share, share.at[c], ag_send, ag_recv)

    def forward(source, slot, k):
        return pltpu.make_async_remote_copy(
            src_ref=source, dst_ref=share.at[c, slot], send_sem=fw_send.at[k], recv_sem=fw_recv.at[k],
            device_id={"row": r, "head": other}, device_id_type=MESH,
        )

    def forwarded(slot, k):
        return pltpu.make_async_remote_copy(
            src_ref=own_share, dst_ref=share.at[other, slot], send_sem=fw_send.at[k], recv_sem=fw_recv.at[k],
            device_id={"row": r, "head": other}, device_id_type=MESH,
        )

    fw_out, fw_back = [forward(own_share, r, 0)], [forwarded(r, 0)]
    fw_out[0].start()
    for k in range(1, rows):
        ag_back[k - 1].wait_recv()
        come = lax.rem(r + rows - k, rows)
        copy = forward(share.at[c, come], come, k)
        copy.start()
        fw_out.append(copy)
        fw_back.append(forwarded(come, k))
    for copy in fw_back:
        copy.wait_recv()

    for i in range(rows):
        for j in range(cores):
            at = (i * cores + j) * width
            joined[:, at : at + width] = share[j, i].astype(jnp.float32)
    full = joined[...]
    scale = lax.rsqrt(jnp.mean(full * full, axis=-1, keepdims=True) + epsilon)
    feat = (full * scale * final_gain[...]).astype(jnp.bfloat16)
    loads[6].wait()
    vocab_here = w_vocab.shape[0]
    logits = dot_nt(feat, wvoc[...])
    entry = lane_of((seqs, vocab_here))
    picked = jnp.sum(jnp.where(entry == targets[...] - spot * vocab_here, logits, 0.0), axis=-1, keepdims=True)
    highest = jnp.max(logits, axis=-1, keepdims=True)
    total = jnp.sum(jnp.exp(logits - highest), axis=-1, keepdims=True)
    small_send[2] = as_rows([highest, total, picked])
    last_in[spot] = small_send[2]
    ls_out, ls_back = [], []
    for k in range(1, rows * cores):
        to = lax.rem(spot + k, rows * cores)
        come = lax.rem(spot + rows * cores - k, rows * cores)
        for slot, kept in ((spot, ls_out), (come, ls_back)):
            kept.append(
                pltpu.make_async_remote_copy(
                    src_ref=small_send.at[2], dst_ref=last_in.at[slot], send_sem=ls_send.at[k],
                    recv_sem=ls_recv.at[k], device_id={"row": to // cores, "head": lax.rem(to, cores)},
                    device_id_type=MESH,
                )
            )
        ls_out[-1].start()
    for copy in v_back:
        copy.wait_recv()
    for copy in ls_back:
        copy.wait_recv()
    top = last_in[0, 0:1]
    for i in range(1, rows * cores):
        top = jnp.maximum(top, last_in[i, 0:1])
    total = jnp.zeros_like(top)
    picked = jnp.zeros_like(top)
    for i in range(rows * cores):
        total = total + last_in[i, 1:2] * jnp.exp(last_in[i, 0:1] - top)
        picked = picked + last_in[i, 2:3]
    log_prob[...] = picked - (top + jnp.log(total))
    for copy in qk_out + rd_out + v_out + st_out + [pair_copy] + pr_out + ag_out + fw_out + ls_out:
        copy.wait_send()


def fused(rows, cores, *args):
    (hidden, norm_gain, w_query, w_key, w_value, w_outgate, w_out, w_gates, gate_bias, headnorm_gain, final_gain,
     w_vocab, memory, normalizer, stabilizer, targets) = args
    seqs, model = hidden.shape
    heads, keys = w_query.shape[:2]
    vals = w_value.shape[1]
    head_dim = memory.shape[3]
    width = model // (rows * cores)
    f32, bf16 = jnp.float32, jnp.bfloat16
    vmem = pl.BlockSpec(memory_space=pltpu.VMEM)
    hbm = pl.BlockSpec(memory_space=pl.ANY)
    places = [vmem, vmem] + [hbm] * 5 + [vmem] * 4 + [hbm] * 2 + [vmem] * 2
    dma = pltpu.SemaphoreType.DMA
    values, key, decay, stabilizer_out, hidden_out, log_prob = pl.pallas_call(
        functools.partial(kernel, rows, cores, heads),
        out_shape=[
            jax.ShapeDtypeStruct((rows, seqs, heads * vals), bf16),
            jax.ShapeDtypeStruct((seqs, heads * keys), f32),
            jax.ShapeDtypeStruct((seqs, heads), f32),
            jax.ShapeDtypeStruct((seqs, heads), f32),
            jax.ShapeDtypeStruct((seqs, width), bf16),
            jax.ShapeDtypeStruct((1, seqs), f32),
        ],
        in_specs=places,
        out_specs=[vmem] * 6,
        scratch_shapes=[
            pltpu.VMEM(w_query.shape, bf16), pltpu.VMEM(w_key.shape, bf16), pltpu.VMEM(w_value.shape, bf16),
            pltpu.VMEM(w_outgate.shape, bf16), pltpu.VMEM(w_out.shape, bf16), pltpu.VMEM(w_vocab.shape, bf16),
            pltpu.VMEM(memory.shape, f32),
            pltpu.VMEM((seqs, heads * keys, LANES), f32),
            pltpu.VMEM((seqs, heads * vals), bf16),
            pltpu.VMEM((heads, seqs, head_dim), f32),
            pltpu.VMEM((rows, seqs, heads * vals), f32),
            pltpu.VMEM((rows, seqs, heads * vals), f32),
            pltpu.VMEM((rows, 8, seqs), f32),
            pltpu.VMEM((rows, 8, seqs), f32),
            pltpu.VMEM((cores, rows, seqs, width), f32),
            pltpu.VMEM((rows, seqs, width), f32),
            pltpu.VMEM((rows, seqs, width), f32),
            pltpu.VMEM((rows, seqs, width), f32),
            pltpu.VMEM((cores, rows, seqs, width), bf16),
            pltpu.VMEM((seqs, width), bf16),
            pltpu.VMEM((seqs, model), f32),
            pltpu.VMEM((rows * cores, 8, seqs), f32),
            pltpu.VMEM((3, 8, seqs), f32),
            dma((7,)),
        ]
        + [dma((rows,))] * 8
        + [dma, dma]
        + [dma((rows,))] * 6
        + [dma((rows * cores,))] * 2,
        compiler_params=pltpu.CompilerParams(
            collective_id=0, has_side_effects=True, vmem_limit_bytes=56 * 1024 * 1024
        ),
    )(
        hidden, norm_gain.reshape(1, model), w_query, w_key, w_value, w_outgate, w_out, w_gates, gate_bias,
        headnorm_gain.reshape(1, heads * vals), final_gain.reshape(1, model), w_vocab, memory, stabilizer,
        targets.reshape(seqs, 1),
    )
    key = key.reshape(seqs, heads, keys)
    value = values.reshape(rows, seqs, heads, vals).transpose(1, 2, 0, 3).reshape(seqs, heads, head_dim)
    memory_out = (
        decay[:, :, None, None] * memory + key[:, :, :, None] * value.astype(f32)[:, :, None, :]
    )
    normalizer_out = decay[:, :, None] * normalizer + key
    return memory_out, normalizer_out, stabilizer_out, hidden_out, log_prob.reshape(seqs)


def joined_2(value, axis, join):
    pieces = jax.tree.map(lambda part: lax.all_gather(part, axis), value)
    head = jax.tree.map(lambda part: part[0], pieces)
    tail = jax.tree.map(lambda part: part[1:], pieces)
    total, _ = lax.scan(lambda total, share: (join(total, share), None), head, tail)
    return total


def rms_round(stream, gain):
    scale = lax.rsqrt(jnp.mean(stream * stream, axis=-1, keepdims=True) + epsilon)
    return (stream * scale * gain).astype(jnp.bfloat16)


def per_device(
    hidden,
    norm_gain,
    w_query,
    w_key,
    w_value,
    w_outgate,
    w_out,
    w_gates,
    gate_bias,
    headnorm_gain,
    final_gain,
    w_vocab,
    memory,
    normalizer,
    stabilizer,
    targets,
):
    value_rows = w_value.shape[1]
    stream = hidden.astype(jnp.float32)
    normed_in = rms_round(stream, norm_gain)

    def project(weights):
        return jnp.einsum("sd,hjd->shj", normed_in, weights, preferred_element_type=jnp.float32)

    queries = project(w_query) / math.sqrt(w_query.shape[1] * lax.axis_size("row"))
    key_part = project(w_key)
    value_part = project(w_value).astype(jnp.bfloat16)
    outgate_pre = project(w_outgate)
    gate_pre = (
        jnp.einsum("sd,ghd->gsh", normed_in, w_gates, preferred_element_type=jnp.float32)
        + gate_bias[:, None, :]
    )
    log_forget = jax.nn.log_sigmoid(gate_pre[1])
    stabilizer_out = jnp.maximum(log_forget + stabilizer, gate_pre[0])
    decay_rate = jnp.exp(log_forget + stabilizer - stabilizer_out)
    inflow = jnp.exp(gate_pre[0] - stabilizer_out)
    scaled_key = inflow[:, :, None] * key_part
    memory_out = (
        decay_rate[:, :, None, None] * memory
        + scaled_key[:, :, :, None]
        * lax.all_gather(value_part, "row", axis=2, tiled=True).astype(jnp.float32)[:, :, None, :]
    )
    normalizer_out = decay_rate[:, :, None] * normalizer + scaled_key
    partial_readout = jnp.einsum(
        "shj,shje->she", queries, memory_out, precision=lax.Precision.HIGHEST
    )
    readout = lax.psum(partial_readout, "row")
    average = jnp.mean(readout, axis=-1)
    centered_full = readout - average[:, :, None]
    variance = jnp.mean(centered_full * centered_full, axis=-1)
    centered = lax.dynamic_slice_in_dim(
        centered_full, lax.axis_index("row") * value_rows, value_rows, 2
    )
    normed = centered * lax.rsqrt(variance + epsilon)[:, :, None] * headnorm_gain
    gated_out = (jax.nn.sigmoid(outgate_pre) * normed).astype(jnp.bfloat16)
    partial_terms = jnp.einsum("shj,hjd->sd", gated_out, w_out, preferred_element_type=jnp.float32)
    position = lax.axis_index("row") * lax.axis_size("head") + lax.axis_index("head")
    share_width = hidden.shape[1] // (lax.axis_size("row") * lax.axis_size("head"))
    vocab_here = w_vocab.shape[0]
    projection = lax.psum(partial_terms, ("row", "head"))
    new_full = (stream + projection).astype(jnp.bfloat16)
    final_feat = rms_round(new_full.astype(jnp.float32), final_gain)
    logits = jnp.einsum("sd,vd->sv", final_feat, w_vocab, preferred_element_type=jnp.float32)
    hidden_out = lax.dynamic_slice_in_dim(new_full, position * share_width, share_width, 1)
    local_ids = targets - position * vocab_here
    is_target = jnp.arange(vocab_here, dtype=jnp.int32)[None, :] == local_ids[:, None]
    target_term = jnp.sum(jnp.where(is_target, logits, 0.0), axis=-1)
    local_max = jnp.max(logits, axis=-1)
    local_sum = jnp.sum(jnp.exp(logits - local_max[:, None]), axis=-1)

    def combine(earlier, later):
        highest = jnp.maximum(earlier[0], later[0])
        joined = earlier[1] * jnp.exp(earlier[0] - highest) + later[1] * jnp.exp(later[0] - highest)
        return (highest, joined, earlier[2] + later[2])

    highest, exp_total, picked = joined_2(
        (local_max, local_sum, target_term), ("row", "head"), combine
    )
    log_prob = picked - (highest + jnp.log(exp_total))
    return (memory_out, normalizer_out, stabilizer_out, hidden_out, log_prob)


def solution(mesh):
    in_specs = (
        P("groups", None),
        P(),
        P("head", "row", None),
        P("head", "row", None),
        P("head", "row", None),
        P("head", "row", None),
        P("head", "row", None),
        P(None, "head", None),
        P(None, "head"),
        P("head", "row"),
        P(),
        P(("row", "head"), None),
        P("groups", "head", "row", None),
        P("groups", "head", "row"),
        P("groups", "head"),
        P("groups"),
    )
    out_specs = (
        P("groups", "head", "row", None),
        P("groups", "head", "row"),
        P("groups", "head"),
        P("groups", ("row", "head")),
        P("groups"),
    )
    rows, cores = mesh.shape["row"], mesh.shape["head"]

    def step(*args):
        model, heads, vals = args[0].shape[1], args[2].shape[0], args[4].shape[1]
        lined_up = 2 * vals == LANES and heads % 2 == 0 and 2 * heads <= 8 and cores == 2
        lined_up = lined_up and args[0].shape[0] % 8 == 0 and heads * args[2].shape[1] == LANES and model % (rows * cores * LANES) == 0
        return fused(rows, cores, *args) if lined_up else per_device(*args)

    return jax.shard_map(
        step, mesh=mesh, in_specs=in_specs, out_specs=out_specs, check_vma=False
    )
```

```python
import functools
import math

import jax
import jax.numpy as jnp
from jax import lax
from jax.experimental import pallas as pl
from jax.experimental.pallas import tpu as pltpu
from jax.sharding import PartitionSpec as P

epsilon = 1e-06
LANES = 128
MESH = pl.DeviceIdType.MESH


def dot_nt(left, right):
    return lax.dot_general(left, right, (((1,), (1,)), ((), ())), preferred_element_type=jnp.float32)


def lane_of(shape):
    return lax.broadcasted_iota(jnp.int32, shape, len(shape) - 1)


def spread(columns, width, count):
    head_of = lane_of((columns.shape[0], width * count)) // width
    total = jnp.zeros((columns.shape[0], width * count), jnp.float32)
    for h in range(count):
        total = jnp.where(head_of == h, columns[:, h : h + 1], total)
    return total


def segment_sums(values, width, count):
    head_of = lane_of(values.shape) // width
    return [jnp.sum(jnp.where(head_of == h, values, 0.0), axis=-1, keepdims=True) for h in range(count)]


def as_rows(columns):
    seqs = columns[0].shape[0]
    lane = lane_of((seqs, LANES))
    wide = jnp.zeros((seqs, LANES), jnp.float32)
    for i, column in enumerate(columns):
        wide = jnp.where(lane == i, column, wide)
    return jnp.transpose(wide)[0:8, :]


def kernel(
    rows, cores, heads,
    hidden, norm_gain, w_query, w_key, w_value, w_outgate, w_out, w_gates, gate_bias, headnorm, final_gain,
    w_vocab, memory, normalizer, stabilizer_t, targets,
    mem, normalizer_out, stabilizer_out, hidden_out, log_prob,
    wq, wk, wv, wg, wo, wvoc, values_out, key_cols, decay_rows, value_rows,
    q_cols, part, readout, read_send, read_in, qk_in, stat_in, proj, pair_in, proj_send, proj_in, share, own_share,
    joined, last_in, small_send,
    load_sem, v_send, v_recv, qk_send, qk_recv, rd_send, rd_recv, st_send, st_recv,
    pa_send, pa_recv, pr_send, pr_recv, ag_send, ag_recv, fw_send, fw_recv, ls_send, ls_recv,
):
    seqs, model = hidden.shape
    r = lax.axis_index("row")
    c = lax.axis_index("head")
    other = 1 - c
    spot = r * cores + c
    keys = w_query.shape[1]
    vals = w_value.shape[1]
    head_dim = memory.shape[3]
    width = share.shape[3]

    loads = [
        pltpu.make_async_copy(source, target, load_sem.at[i])
        for i, (source, target) in enumerate(
            ((w_key, wk), (w_query, wq), (memory, mem), (w_value, wv), (w_outgate, wg), (w_out, wo), (w_vocab, wvoc))
        )
    ]
    for i in (0, 1, 3, 2, 4):
        loads[i].start()

    barrier = pltpu.get_barrier_semaphore()
    for k in range(1, rows * cores):
        to = lax.rem(spot + k, rows * cores)
        pl.semaphore_signal(
            barrier, inc=1, device_id={"row": to // cores, "head": lax.rem(to, cores)}, device_id_type=MESH
        )

    def to_rows(source_of, target, send, recv):
        out, back = [], []
        for k in range(1, rows):
            to = lax.rem(r + k, rows)
            come = lax.rem(r + rows - k, rows)
            where = {"row": to, "head": c}
            copy = pltpu.make_async_remote_copy(
                src_ref=source_of(to), dst_ref=target.at[r], send_sem=send.at[k], recv_sem=recv.at[k],
                device_id=where, device_id_type=MESH,
            )
            copy.start()
            out.append(copy)
            back.append(
                pltpu.make_async_remote_copy(
                    src_ref=source_of(to), dst_ref=target.at[come], send_sem=send.at[k], recv_sem=recv.at[k],
                    device_id=where, device_id_type=MESH,
                )
            )
        return out, back

    stabilizer = jnp.transpose(jnp.concatenate([stabilizer_t[...]] * (LANES // heads), axis=0))[:, 0:heads]
    wanted = jnp.transpose(jnp.broadcast_to(targets[...].astype(jnp.float32), (LANES, seqs)))[:, 0:1].astype(jnp.int32)
    gain_rows = jnp.concatenate([headnorm[h : h + 1, :] for h in range(heads)], axis=1)
    stream = hidden[...].astype(jnp.float32)
    scale = lax.rsqrt(jnp.mean(stream * stream, axis=-1, keepdims=True) + epsilon)
    x = (stream * scale * norm_gain[...]).astype(jnp.bfloat16)
    gate_in = dot_nt(x, w_gates[0]) + gate_bias[0:1, :]
    gate_forget = dot_nt(x, w_gates[1]) + gate_bias[1:2, :]
    log_forget = jnp.minimum(gate_forget, 0.0) - jnp.log1p(jnp.exp(-jnp.abs(gate_forget)))
    top = jnp.maximum(log_forget + stabilizer, gate_in)
    decay = jnp.exp(log_forget + stabilizer - top)
    inflow = jnp.exp(gate_in - top)
    stabilizer_out[...] = as_rows([top[:, h : h + 1] for h in range(heads)])[0:heads]
    for h in range(heads):
        decay_rows[h] = jnp.broadcast_to(decay[:, h : h + 1], (seqs, LANES))

    loads[0].wait()
    key = dot_nt(x, wk[...].reshape(heads * keys, model)) * spread(inflow, keys, heads)
    for h in range(heads):
        normalizer_out[:, h, :] = decay[:, h : h + 1] * normalizer[:, h, :] + key[:, h * keys : (h + 1) * keys]
    key_t = jnp.transpose(key)
    loads[1].wait()
    query = dot_nt(x, wq[...].reshape(heads * keys, model)) / math.sqrt(rows * keys)
    query_t = jnp.transpose(query)
    for s in range(seqs):
        q_cols[s] = jnp.broadcast_to(query_t[:, s : s + 1], (heads * keys, LANES))
        key_cols[s] = jnp.broadcast_to(key_t[:, s : s + 1], (heads * keys, LANES))
    small_send[0] = as_rows(segment_sums(query * key, keys, heads))
    qk_in[r] = small_send[0]
    pl.semaphore_wait(barrier, rows * cores - 1)
    qk_out, qk_back = to_rows(lambda to: small_send.at[0], qk_in, qk_send, qk_recv)

    loads[3].wait()
    value = dot_nt(x, wv[...].reshape(heads * vals, model)).astype(jnp.bfloat16)
    part[...] = value
    values_out[r] = value
    v_out, v_back = to_rows(lambda to: part, values_out, v_send, v_recv)

    loads[2].wait()

    sublane = lax.broadcasted_iota(jnp.int32, (8, LANES), 0)

    def read(group, carry):
        for h in range(heads):
            for t in range(head_dim // LANES):
                stack = jnp.zeros((8, LANES), jnp.float32)
                for i in range(8):
                    s = group * 8 + i
                    q = q_cols[s, h * keys : (h + 1) * keys, :]
                    block = mem[s, h, :, t * LANES : (t + 1) * LANES]
                    stack = jnp.where(sublane == i, jnp.sum(q * block, axis=0, keepdims=True), stack)
                first = pl.multiple_of(group * 8, 8)
                readout[h, pl.ds(first, 8), t * LANES : (t + 1) * LANES] = stack
        return carry

    lax.fori_loop(0, seqs // 8, read, 0)
    low = lane_of((seqs, LANES)) < vals
    for pair in range(heads // 2):
        for t in range(head_dim // LANES):
            tile = slice(t * LANES, (t + 1) * LANES)
            a = readout[2 * pair, :, tile] * decay[:, 2 * pair : 2 * pair + 1]
            b = readout[2 * pair + 1, :, tile] * decay[:, 2 * pair + 1 : 2 * pair + 2]
            here = slice(pair * LANES, (pair + 1) * LANES)
            read_send[2 * t, :, here] = jnp.where(low, a, pltpu.roll(b, vals, 1))
            read_send[2 * t + 1, :, here] = jnp.where(low, pltpu.roll(a, vals, 1), b)
    read_in[r] = read_send[r]
    rd_out, rd_back = to_rows(lambda to: read_send.at[to], read_in, rd_send, rd_recv)

    loads[5].start()
    loads[6].start()
    loads[4].wait()
    gate = jax.nn.sigmoid(dot_nt(x, wg[...].reshape(heads * vals, model)))

    for copy in v_back:
        copy.wait_recv()
    for h in range(heads):
        here = slice((h // 2) * LANES, (h // 2 + 1) * LANES)
        for t in range(head_dim // LANES):
            a = values_out[2 * t, :, here].astype(jnp.float32)
            b = values_out[2 * t + 1, :, here].astype(jnp.float32)
            if h % 2:
                a = pltpu.roll(a, vals, 1)
            else:
                b = pltpu.roll(b, vals, 1)
            value_rows[h, :, t * LANES : (t + 1) * LANES] = jnp.where(low, a, b)

    def update(group, carry):
        first = pl.multiple_of(group * 8, 8)
        for h in range(heads):
            keep = decay_rows[h, pl.ds(first, 8), :]
            for t in range(head_dim // LANES):
                tile = slice(t * LANES, (t + 1) * LANES)
                fresh = value_rows[h, pl.ds(first, 8), tile]
                for i in range(8):
                    s = group * 8 + i
                    old = mem[s, h, :, tile]
                    column = key_cols[s, h * keys : (h + 1) * keys, :]
                    mem[s, h, :, tile] = keep[i : i + 1] * old + column * fresh[i : i + 1]
        return carry

    lax.fori_loop(0, seqs // 8, update, 0)
    for copy in qk_back:
        copy.wait_recv()
    qk_rows = qk_in[0]
    for i in range(1, rows):
        qk_rows = qk_rows + qk_in[i]
    qk = jnp.transpose(jnp.concatenate([qk_rows] + [jnp.zeros_like(qk_rows)] * (LANES // 8 - 1), axis=0))
    value_term = spread(qk, vals, heads) * value.astype(jnp.float32)

    for copy in rd_back:
        copy.wait_recv()
    read_full = value_term
    for i in range(rows):
        read_full = read_full + read_in[i]
    means = [total / vals for total in segment_sums(read_full, vals, heads)]
    local_mean = spread(jnp.concatenate(means, axis=1), vals, heads)
    offs = read_full - local_mean
    small_send[1] = as_rows(means + segment_sums(offs * offs, vals, heads))
    stat_in[r] = small_send[1]
    st_out, st_back = to_rows(lambda to: small_send.at[1], stat_in, st_send, st_recv)
    for copy in st_back:
        copy.wait_recv()
    average = stat_in[0, 0:heads]
    spreads = stat_in[0, heads : 2 * heads]
    for i in range(1, rows):
        average = average + stat_in[i, 0:heads]
        spreads = spreads + stat_in[i, heads : 2 * heads]
    average = average / rows
    for i in range(rows):
        off = stat_in[i, 0:heads] - average
        spreads = spreads + vals * off * off
    inverse = lax.rsqrt(spreads / head_dim + epsilon)
    both = jnp.concatenate([average, inverse], axis=0)
    both = jnp.transpose(jnp.concatenate([both] + [jnp.zeros_like(both)] * (LANES // 8 - 1), axis=0))
    normed = (read_full - spread(both, vals, heads)) * spread(both[:, heads:], vals, heads) * gain_rows
    gated = (gate * normed).astype(jnp.bfloat16)

    loads[5].wait()
    for i in range(rows):
        for j in range(cores):
            at = (i * cores + j) * width
            proj[j, i] = jnp.dot(
                gated, wo[:, :, at : at + width].reshape(heads * vals, width), preferred_element_type=jnp.float32
            )
    pair_copy = pltpu.make_async_remote_copy(
        src_ref=proj.at[other], dst_ref=pair_in, send_sem=pa_send, recv_sem=pa_recv,
        device_id={"row": r, "head": other}, device_id_type=MESH,
    )
    pair_copy.start()
    pair_copy.wait_recv()
    for i in range(rows):
        proj_send[i] = proj[c, i] + pair_in[i]
    proj_in[r] = proj_send[r]
    pr_out, pr_back = to_rows(lambda to: proj_send.at[to], proj_in, pr_send, pr_recv)
    for copy in pr_back:
        copy.wait_recv()
    new = proj_in[0]
    for i in range(1, rows):
        new = new + proj_in[i]
    mine = hidden[:, pl.ds(pl.multiple_of(spot * width, LANES), width)].astype(jnp.float32)
    new = (mine + new).astype(jnp.bfloat16)
    hidden_out[...] = new
    own_share[...] = new
    share[c, r] = new
    ag_out, ag_back = to_rows(lambda to: own_share, share.at[c], ag_send, ag_recv)

    def forward(source, slot, k):
        return pltpu.make_async_remote_copy(
            src_ref=source, dst_ref=share.at[c, slot], send_sem=fw_send.at[k], recv_sem=fw_recv.at[k],
            device_id={"row": r, "head": other}, device_id_type=MESH,
        )

    def forwarded(slot, k):
        return pltpu.make_async_remote_copy(
            src_ref=own_share, dst_ref=share.at[other, slot], send_sem=fw_send.at[k], recv_sem=fw_recv.at[k],
            device_id={"row": r, "head": other}, device_id_type=MESH,
        )

    fw_out, fw_back = [forward(own_share, r, 0)], [forwarded(r, 0)]
    fw_out[0].start()
    for k in range(1, rows):
        ag_back[k - 1].wait_recv()
        come = lax.rem(r + rows - k, rows)
        copy = forward(share.at[c, come], come, k)
        copy.start()
        fw_out.append(copy)
        fw_back.append(forwarded(come, k))
    for copy in fw_back:
        copy.wait_recv()

    for i in range(rows):
        for j in range(cores):
            at = (i * cores + j) * width
            joined[:, at : at + width] = share[j, i].astype(jnp.float32)
    full = joined[...]
    scale = lax.rsqrt(jnp.mean(full * full, axis=-1, keepdims=True) + epsilon)
    feat = (full * scale * final_gain[...]).astype(jnp.bfloat16)
    loads[6].wait()
    vocab_here = w_vocab.shape[0]
    logits = dot_nt(feat, wvoc[...])
    entry = lane_of((seqs, vocab_here))
    picked = jnp.sum(jnp.where(entry == wanted - spot * vocab_here, logits, 0.0), axis=-1, keepdims=True)
    highest = jnp.max(logits, axis=-1, keepdims=True)
    total = jnp.sum(jnp.exp(logits - highest), axis=-1, keepdims=True)
    small_send[2] = as_rows([highest, total, picked])
    last_in[spot] = small_send[2]
    ls_out, ls_back = [], []
    for k in range(1, rows * cores):
        to = lax.rem(spot + k, rows * cores)
        come = lax.rem(spot + rows * cores - k, rows * cores)
        for slot, kept in ((spot, ls_out), (come, ls_back)):
            kept.append(
                pltpu.make_async_remote_copy(
                    src_ref=small_send.at[2], dst_ref=last_in.at[slot], send_sem=ls_send.at[k],
                    recv_sem=ls_recv.at[k], device_id={"row": to // cores, "head": lax.rem(to, cores)},
                    device_id_type=MESH,
                )
            )
        ls_out[-1].start()
    for copy in ls_back:
        copy.wait_recv()
    top = last_in[0, 0:1]
    for i in range(1, rows * cores):
        top = jnp.maximum(top, last_in[i, 0:1])
    total = jnp.zeros_like(top)
    picked = jnp.zeros_like(top)
    for i in range(rows * cores):
        total = total + last_in[i, 1:2] * jnp.exp(last_in[i, 0:1] - top)
        picked = picked + last_in[i, 2:3]
    log_prob[...] = picked - (top + jnp.log(total))
    for copy in qk_out + rd_out + v_out + st_out + [pair_copy] + pr_out + ag_out + fw_out + ls_out:
        copy.wait_send()


def fused(rows, cores, *args):
    (hidden, norm_gain, w_query, w_key, w_value, w_outgate, w_out, w_gates, gate_bias, headnorm_gain, final_gain,
     w_vocab, memory, normalizer, stabilizer, targets) = args
    seqs, model = hidden.shape
    heads, keys = w_query.shape[:2]
    vals = w_value.shape[1]
    head_dim = memory.shape[3]
    width = model // (rows * cores)
    f32, bf16 = jnp.float32, jnp.bfloat16
    vmem = pl.BlockSpec(memory_space=pltpu.VMEM)
    hbm = pl.BlockSpec(memory_space=pl.ANY)
    places = [vmem, vmem] + [hbm] * 5 + [vmem] * 4 + [hbm] * 2 + [vmem] * 3
    dma = pltpu.SemaphoreType.DMA
    memory_out, normalizer_out, stabilizer_out, hidden_out, log_prob = pl.pallas_call(
        functools.partial(kernel, rows, cores, heads),
        out_shape=[
            pltpu.VMEM(memory.shape, f32),
            jax.ShapeDtypeStruct(normalizer.shape, f32),
            jax.ShapeDtypeStruct((heads, seqs), f32),
            jax.ShapeDtypeStruct((seqs, width), bf16),
            jax.ShapeDtypeStruct((1, seqs), f32),
        ],
        in_specs=places,
        out_specs=[vmem] * 5,
        scratch_shapes=[
            pltpu.VMEM(w_query.shape, bf16), pltpu.VMEM(w_key.shape, bf16), pltpu.VMEM(w_value.shape, bf16),
            pltpu.VMEM(w_outgate.shape, bf16), pltpu.VMEM(w_out.shape, bf16), pltpu.VMEM(w_vocab.shape, bf16),
            pltpu.VMEM((rows, seqs, heads * vals), bf16),
            pltpu.VMEM((seqs, heads * keys, LANES), f32),
            pltpu.VMEM((heads, seqs, LANES), f32),
            pltpu.VMEM((heads, seqs, head_dim), f32),
            pltpu.VMEM((seqs, heads * keys, LANES), f32),
            pltpu.VMEM((seqs, heads * vals), bf16),
            pltpu.VMEM((heads, seqs, head_dim), f32),
            pltpu.VMEM((rows, seqs, heads * vals), f32),
            pltpu.VMEM((rows, seqs, heads * vals), f32),
            pltpu.VMEM((rows, 8, seqs), f32),
            pltpu.VMEM((rows, 8, seqs), f32),
            pltpu.VMEM((cores, rows, seqs, width), f32),
            pltpu.VMEM((rows, seqs, width), f32),
            pltpu.VMEM((rows, seqs, width), f32),
            pltpu.VMEM((rows, seqs, width), f32),
            pltpu.VMEM((cores, rows, seqs, width), bf16),
            pltpu.VMEM((seqs, width), bf16),
            pltpu.VMEM((seqs, model), f32),
            pltpu.VMEM((rows * cores, 8, seqs), f32),
            pltpu.VMEM((3, 8, seqs), f32),
            dma((7,)),
        ]
        + [dma((rows,))] * 8
        + [dma, dma]
        + [dma((rows,))] * 6
        + [dma((rows * cores,))] * 2,
        compiler_params=pltpu.CompilerParams(
            collective_id=0, has_side_effects=True, vmem_limit_bytes=48 * 1024 * 1024
        ),
    )(
        hidden, norm_gain.reshape(1, model), w_query, w_key, w_value, w_outgate, w_out, w_gates, gate_bias,
        headnorm_gain, final_gain.reshape(1, model), w_vocab, memory, normalizer, stabilizer.T,
        targets.reshape(1, seqs),
    )
    return memory_out, normalizer_out, stabilizer_out.T, hidden_out, log_prob.reshape(seqs)


def joined_2(value, axis, join):
    pieces = jax.tree.map(lambda part: lax.all_gather(part, axis), value)
    head = jax.tree.map(lambda part: part[0], pieces)
    tail = jax.tree.map(lambda part: part[1:], pieces)
    total, _ = lax.scan(lambda total, share: (join(total, share), None), head, tail)
    return total


def rms_round(stream, gain):
    scale = lax.rsqrt(jnp.mean(stream * stream, axis=-1, keepdims=True) + epsilon)
    return (stream * scale * gain).astype(jnp.bfloat16)


def per_device(
    hidden,
    norm_gain,
    w_query,
    w_key,
    w_value,
    w_outgate,
    w_out,
    w_gates,
    gate_bias,
    headnorm_gain,
    final_gain,
    w_vocab,
    memory,
    normalizer,
    stabilizer,
    targets,
):
    value_rows = w_value.shape[1]
    stream = hidden.astype(jnp.float32)
    normed_in = rms_round(stream, norm_gain)

    def project(weights):
        return jnp.einsum("sd,hjd->shj", normed_in, weights, preferred_element_type=jnp.float32)

    queries = project(w_query) / math.sqrt(w_query.shape[1] * lax.axis_size("row"))
    key_part = project(w_key)
    value_part = project(w_value).astype(jnp.bfloat16)
    outgate_pre = project(w_outgate)
    gate_pre = (
        jnp.einsum("sd,ghd->gsh", normed_in, w_gates, preferred_element_type=jnp.float32)
        + gate_bias[:, None, :]
    )
    log_forget = jax.nn.log_sigmoid(gate_pre[1])
    stabilizer_out = jnp.maximum(log_forget + stabilizer, gate_pre[0])
    decay_rate = jnp.exp(log_forget + stabilizer - stabilizer_out)
    inflow = jnp.exp(gate_pre[0] - stabilizer_out)
    scaled_key = inflow[:, :, None] * key_part
    memory_out = (
        decay_rate[:, :, None, None] * memory
        + scaled_key[:, :, :, None]
        * lax.all_gather(value_part, "row", axis=2, tiled=True).astype(jnp.float32)[:, :, None, :]
    )
    normalizer_out = decay_rate[:, :, None] * normalizer + scaled_key
    partial_readout = jnp.einsum(
        "shj,shje->she", queries, memory_out, precision=lax.Precision.HIGHEST
    )
    readout = lax.psum(partial_readout, "row")
    average = jnp.mean(readout, axis=-1)
    centered_full = readout - average[:, :, None]
    variance = jnp.mean(centered_full * centered_full, axis=-1)
    centered = lax.dynamic_slice_in_dim(
        centered_full, lax.axis_index("row") * value_rows, value_rows, 2
    )
    normed = centered * lax.rsqrt(variance + epsilon)[:, :, None] * headnorm_gain
    gated_out = (jax.nn.sigmoid(outgate_pre) * normed).astype(jnp.bfloat16)
    partial_terms = jnp.einsum("shj,hjd->sd", gated_out, w_out, preferred_element_type=jnp.float32)
    position = lax.axis_index("row") * lax.axis_size("head") + lax.axis_index("head")
    share_width = hidden.shape[1] // (lax.axis_size("row") * lax.axis_size("head"))
    vocab_here = w_vocab.shape[0]
    projection = lax.psum(partial_terms, ("row", "head"))
    new_full = (stream + projection).astype(jnp.bfloat16)
    final_feat = rms_round(new_full.astype(jnp.float32), final_gain)
    logits = jnp.einsum("sd,vd->sv", final_feat, w_vocab, preferred_element_type=jnp.float32)
    hidden_out = lax.dynamic_slice_in_dim(new_full, position * share_width, share_width, 1)
    local_ids = targets - position * vocab_here
    is_target = jnp.arange(vocab_here, dtype=jnp.int32)[None, :] == local_ids[:, None]
    target_term = jnp.sum(jnp.where(is_target, logits, 0.0), axis=-1)
    local_max = jnp.max(logits, axis=-1)
    local_sum = jnp.sum(jnp.exp(logits - local_max[:, None]), axis=-1)

    def combine(earlier, later):
        highest = jnp.maximum(earlier[0], later[0])
        joined = earlier[1] * jnp.exp(earlier[0] - highest) + later[1] * jnp.exp(later[0] - highest)
        return (highest, joined, earlier[2] + later[2])

    highest, exp_total, picked = joined_2(
        (local_max, local_sum, target_term), ("row", "head"), combine
    )
    log_prob = picked - (highest + jnp.log(exp_total))
    return (memory_out, normalizer_out, stabilizer_out, hidden_out, log_prob)


def solution(mesh):
    in_specs = (
        P("groups", None),
        P(),
        P("head", "row", None),
        P("head", "row", None),
        P("head", "row", None),
        P("head", "row", None),
        P("head", "row", None),
        P(None, "head", None),
        P(None, "head"),
        P("head", "row"),
        P(),
        P(("row", "head"), None),
        P("groups", "head", "row", None),
        P("groups", "head", "row"),
        P("groups", "head"),
        P("groups"),
    )
    out_specs = (
        P("groups", "head", "row", None),
        P("groups", "head", "row"),
        P("groups", "head"),
        P("groups", ("row", "head")),
        P("groups"),
    )
    rows, cores = mesh.shape["row"], mesh.shape["head"]

    def step(*args):
        model, heads, vals = args[0].shape[1], args[2].shape[0], args[4].shape[1]
        lined_up = 2 * vals == LANES and heads % 2 == 0 and 2 * heads <= 8 and cores == 2
        lined_up = lined_up and args[0].shape[0] % 8 == 0 and heads * args[2].shape[1] == LANES and model % (rows * cores * LANES) == 0
        return fused(rows, cores, *args) if lined_up else per_device(*args)

    return jax.shard_map(
        step, mesh=mesh, in_specs=in_specs, out_specs=out_specs, check_vma=False
    )
```
